512 devices in a mesh: gz: 256 (over x, z, y), col: 2 (over core).
Axes of the slice: x: 4, y: 8, z: 8, core: 2. Of those that a mesh axis runs over, the one named last changes fastest.
Arguments:
- velocity: float32 [1024, 3, 128, 128], P('gz', None, 'col'), may hold values from -6 to 6
- forces: float32 [3, 2097152], P(None, ('gz', 'col')), may hold values from -60 to 60
- offsets: float32 [3, 2097152], P(None, ('gz', 'col')), may hold values from 0 to 1
- cell_x: int32 [2097152], P(('gz', 'col')), may hold values from 0 to 127
- cell_y: int32 [2097152], P(('gz', 'col')), may hold values from 0 to 127
- cell_z: int32 [2097152], P(('gz', 'col')), may hold values from 0 to 12
- band_start: int32 [256], P('gz'), may hold values from 0 to 255, as said below
Outputs:
- force_field: float32 [1024, 3, 128, 128], P('gz', None, 'col')
- velocity_next: float32 [1024, 3, 128, 128], P('gz', None, 'col')
The draws below stay inside these ranges and needn't reach their ends.
Inputs may be any that keep to these rules, and one draw needn't show every extreme that they name: (g - band_start[g]) mod 256 lies in 0 to 3 for every gz index g.
All inputs are finite; a program needn't handle non-finite values.
Results may differ from the reference program's by a relative error of at most 0.0037.
Values sent between devices are 32-bit elements; how exact they have to be, the bound alone decides.
No kernel may reach another device: no remote copies, remote signals or barrier semaphores. Data moves between devices by JAX's collectives and lax.ppermute only.
A program may use at most 64 MiB of HBM per device.

```python
import jax
import jax.numpy as jnp
from jax import lax

CZ = 4
NX = 128
NY = 128
MK_DEV = 4096
BAND = 4
BANDZ = 16
NZ = 1024
MARKERS = 2097152
N_GZ = 256
N_COL = 2


def draw_band_start(key, part):
    backward = jax.random.randint(key, (N_GZ,), 0, BAND)
    backward = backward.at[0].set(0).at[1].set(BAND - 1)
    return ((jnp.arange(N_GZ, dtype=jnp.int32) - backward) % N_GZ).astype(jnp.int32)


def with_ends(entries, key, smallest, high):
    spot = [jax.random.randint(jax.random.fold_in(key, axis), (), 0, length) for axis, length in enumerate(entries.shape)]
    longest = entries.shape.index(max(entries.shape))
    next_to = spot[:longest] + [(spot[longest] + 1) % entries.shape[longest]] + spot[longest + 1:]
    return entries.at[tuple(spot)].set(smallest).at[tuple(next_to)].set(high)


def levels(own_key, extent, shards, least, largest):
    factor_of, own = 1.0, jax.random.fold_in(own_key, 6)
    for position, shards_of in shards:
        steps = jnp.exp(jax.random.uniform(jax.random.fold_in(own, position), (shards_of,), jnp.float32, least / len(shards), largest / len(shards)))
        factor_of = factor_of * jnp.repeat(steps, extent[position] // shards_of).reshape([-1 if axis == position else 1 for axis in range(len(extent))])
    return factor_of


def normal_values(rng, dims, scale, reach, cuts=(), held_as=jnp.bfloat16):
    result = jax.random.normal(rng, dims, jnp.float32) * scale
    if len(cuts) > 0:
        result = levels(rng, dims, cuts, -0.22, 0.18) * result
    return jnp.clip(result, min=-reach, max=reach).astype(held_as)


def setup_inputs(seed: int = 0) -> dict:
    arg_keys = jax.random.split(jax.random.key(seed), 8)
    velocity = normal_values(arg_keys[0], (NZ, 3, NX, NY), 1.0, 6.0, ((0, 256), (2, 2)), jnp.float32)
    forces = normal_values(arg_keys[1], (3, MARKERS), 10.0, 60.0, ((1, 512),), jnp.float32)
    offsets = jnp.clip(1.0 * jax.random.uniform(arg_keys[2], (3, MARKERS), jnp.float32) ** levels(arg_keys[2], (3, MARKERS), ((1, 512),), -0.2, 0.2), 0.0, 1.0)
    cell_x = with_ends(jax.random.randint(arg_keys[3], (MARKERS,), 0, NX), jax.random.fold_in(arg_keys[3], 1), 0, NX - 1).astype(jnp.int32)
    cell_y = with_ends(jax.random.randint(arg_keys[4], (MARKERS,), 0, NY), jax.random.fold_in(arg_keys[4], 1), 0, NY - 1).astype(jnp.int32)
    cell_z = with_ends(jax.random.randint(arg_keys[5], (MARKERS,), 0, BANDZ - 3), jax.random.fold_in(arg_keys[5], 1), 0, (BANDZ - 3) - 1).astype(jnp.int32)
    band_start = draw_band_start(jax.random.fold_in(arg_keys[7], 71), 0)
    return dict(velocity=velocity, forces=forces, offsets=offsets, cell_x=cell_x, cell_y=cell_y, cell_z=cell_z, band_start=band_start)


def delta_weights(fraction):
    root_term = jnp.sqrt(1.0 + 4.0 * fraction - 4.0 * fraction * fraction)
    return jnp.stack([(3.0 - 2.0 * fraction - root_term) / 8.0, (3.0 - 2.0 * fraction + root_term) / 8.0, (1.0 + 2.0 * fraction + root_term) / 8.0, (1.0 + 2.0 * fraction - root_term) / 8.0])

def reference(velocity, forces, offsets, cell_x, cell_y, cell_z, band_start):
    owners = jnp.repeat(band_start, MK_DEV * N_COL)
    z_base = owners * CZ + cell_z
    x_weights = delta_weights(offsets[0])
    y_weights = delta_weights(offsets[1]).T
    z_weights = delta_weights(offsets[2])
    y_rounded = lax.optimization_barrier(y_weights.astype(jnp.bfloat16)).astype(jnp.float32)
    y_index = jnp.stack([(cell_y + corner) % NY for corner in range(4)], axis=1).astype(jnp.int32)
    components = jnp.arange(3, dtype=jnp.int32)
    force_t = forces.T
    field = jnp.zeros((NZ, 3, NX, NY), jnp.float32)
    for z_corner in range(4):
        z_index = ((z_base + z_corner) % NZ).astype(jnp.int32)
        for x_corner in range(4):
            x_index = ((cell_x + x_corner) % NX).astype(jnp.int32)
            scaled = z_weights[z_corner][:, None] * force_t * x_weights[x_corner][:, None]
            scaled = lax.optimization_barrier(scaled.astype(jnp.bfloat16)).astype(jnp.float32)
            values = scaled[:, :, None] * y_rounded[:, None, :]
            field = field.at[z_index[:, None, None], components[None, :, None], x_index[:, None, None], y_index[:, None, :]].add(values)
    neighbours = jnp.roll(velocity, 1, 0) + jnp.roll(velocity, -1, 0)
    neighbours = neighbours + jnp.roll(velocity, 1, 2) + jnp.roll(velocity, -1, 2)
    neighbours = neighbours + jnp.roll(velocity, 1, 3) + jnp.roll(velocity, -1, 3)
    velocity_next = velocity + 0.15 * (neighbours - 6.0 * velocity) + field
    return (field, velocity_next)
```

```python
import jax
import jax.numpy as jnp
from jax import lax
from jax.experimental import pallas as pl
from jax.experimental.pallas import tpu as pltpu
from jax.sharding import PartitionSpec as P

viscous = 0.15
ROWS = 32
ATTRS = 9
LIST = ROWS * ATTRS
KROWS = 4


def vmem():
    return pl.BlockSpec(memory_space=pltpu.VMEM)


def smem():
    return pl.BlockSpec(memory_space=pltpu.SMEM)


def corner_weights(t):
    q = jnp.sqrt(1.0 + 4.0 * t - 4.0 * t * t)
    return (
        (3.0 - 2.0 * t - q) / 8.0,
        (3.0 - 2.0 * t + q) / 8.0,
        (1.0 + 2.0 * t + q) / 8.0,
        (1.0 + 2.0 * t - q) / 8.0,
    )


def prepare(list_ref, base, first_plane, depth, span_x, span_y, span_z, rows_ref):
    def attr(a):
        return list_ref[pl.ds(base + a * ROWS, ROWS), :]

    def put(slot, value):
        rows_ref[pl.ds(slot * ROWS, ROWS), :] = value

    cx, cy = attr(6), attr(7)
    wx, wy, wz = corner_weights(attr(3)), corner_weights(attr(4)), corner_weights(attr(5))
    for b in range(4):
        tx, ty = cx + float(b), cy + float(b)
        put(b, jnp.where(tx >= float(span_x), tx - float(span_x), tx))
        put(4 + b, wx[b])
        put(8 + b, jnp.where(ty >= float(span_y), ty - float(span_y), ty))
        put(12 + b, wy[b].astype(jnp.bfloat16).astype(jnp.float32))
    rel = attr(8) - first_plane
    half = float(span_z // 2)
    rel = jnp.where(rel >= half, rel - float(span_z), rel)
    rel = jnp.where(rel < -half, rel + float(span_z), rel)
    for z in range(depth):
        plane = jnp.zeros_like(rel)
        for a in range(4):
            plane = jnp.where(rel == float(z - a), wz[a], plane)
        put(16 + z, plane)


def build(list_ref, base, rows_ref, row, depth, span_x, span_y, a_ref, b_ref):
    x_at = lax.broadcasted_iota(jnp.int32, (span_x, 128), 0).astype(jnp.float32)
    y_at = lax.broadcasted_iota(jnp.int32, (span_y, 128), 0).astype(jnp.float32)
    for r in range(KROWS):
        lanes = pl.ds(r * 128, 128)

        def get(slot):
            return rows_ref[pl.ds(slot * ROWS + row + r, 1), :]

        wx = jnp.zeros((span_x, 128), jnp.float32)
        wy = jnp.zeros((span_y, 128), jnp.float32)
        for b in range(4):
            wx = jnp.where(x_at == get(b), get(4 + b), wx)
            wy = jnp.where(y_at == get(8 + b), get(12 + b), wy)
        for c in range(3):
            force = list_ref[pl.ds(base + c * ROWS + row + r, 1), :]
            a_ref[pl.ds(c * span_x, span_x), lanes] = (wx * force).astype(jnp.bfloat16)
        for z in range(depth):
            b_ref[pl.ds(z * span_y, span_y), lanes] = (wy * get(16 + z)).astype(jnp.bfloat16)


def spread_list(list_ref, base, first_plane, acc_ref, dims, rows_ref, bufs):
    depth, span_x, span_y, span_z = dims
    turns = ROWS // KROWS
    prepare(list_ref, base, first_plane, depth, span_x, span_y, span_z, rows_ref)

    def fill(turn, which):
        build(list_ref, base, rows_ref, turn * KROWS, depth, span_x, span_y, *bufs[which])

    def add(which):
        a_ref, b_ref = bufs[which]
        out = lax.dot_general(
            a_ref[...], b_ref[...], (((1,), (1,)), ((), ())), preferred_element_type=jnp.float32
        )
        for z in range(depth):
            acc_ref[z] += out[:, z * span_y : (z + 1) * span_y]

    fill(0, 0)

    def two_turns(i, carry):
        fill(2 * i + 1, 1)
        add(0)
        fill(jnp.minimum(2 * i + 2, turns - 1), 0)
        add(1)
        return carry

    lax.fori_loop(0, turns // 2, two_turns, 0)


def scratch(dims):
    depth, span_x, span_y, _ = dims
    a = pltpu.VMEM((3 * span_x, KROWS * 128), jnp.bfloat16)
    b = pltpu.VMEM((depth * span_y, KROWS * 128), jnp.bfloat16)
    return [pltpu.VMEM((20 * ROWS, 128), jnp.float32), a, b, a, b]


def spread(markers, acc, plane, dims):
    depth, span_x, span_y, _ = dims
    lists = markers.shape[0] // LIST

    def kernel(*refs):
        if acc is None:
            plane_ref, list_ref, out_ref, rows_ref, a0, b0, a1, b1 = refs
            out_ref[...] = jnp.zeros_like(out_ref)
        else:
            plane_ref, list_ref, in_ref, out_ref, rows_ref, a0, b0, a1, b1 = refs
            out_ref[...] = in_ref[...]
        for n in range(lists):
            spread_list(list_ref, n * LIST, plane_ref[0], out_ref, dims, rows_ref, ((a0, b0), (a1, b1)))

    operands = (plane, markers) if acc is None else (plane, markers, acc)
    return pl.pallas_call(
        kernel,
        out_shape=jax.ShapeDtypeStruct((depth, 3 * span_x, span_y), jnp.float32),
        in_specs=[smem()] + [vmem()] * (len(operands) - 1),
        out_specs=vmem(),
        scratch_shapes=scratch(dims),
        cost_estimate=pl.CostEstimate(
            flops=lists * 4096 * 3 * span_x * depth * span_y * 2, bytes_accessed=2000000, transcendentals=0
        ),
        name="spread",
    )(*operands)


def by_core(x, gz_count, by):
    pairs = []
    for g in range(gz_count):
        pairs.append((2 * g, 2 * ((g + by) % gz_count)))
        pairs.append((2 * g + 1, 2 * ((g - by) % gz_count) + 1))
    return lax.ppermute(x, ("gz", "col"), pairs)


def on_device(velocity, forces, offsets, cell_x, cell_y, cell_z, band_start):
    depth, _, half_x, span_y = velocity.shape
    gz_count = lax.axis_size("gz")
    gz_index = lax.axis_index("gz")
    col = lax.axis_index("col")
    span_x = half_x * lax.axis_size("col")
    dims = (depth, span_x, span_y, gz_count * depth)
    z_base = (band_start[0] * depth + cell_z).astype(jnp.float32)
    markers = jnp.concatenate(
        [
            forces.reshape(3 * ROWS, 128),
            offsets.reshape(3 * ROWS, 128),
            cell_x.astype(jnp.float32).reshape(ROWS, 128),
            cell_y.astype(jnp.float32).reshape(ROWS, 128),
            z_base.reshape(ROWS, 128),
        ]
    )
    plane_rows = 3 * half_x
    first, last = velocity[0].reshape(plane_rows, span_y), velocity[-1].reshape(plane_rows, span_y)
    mine_out = jnp.where(col == 0, last, first)
    other_out = jnp.where(col == 0, first, last)
    x_low = velocity[:, :, 0].reshape(3 * depth, span_y)
    x_high = velocity[:, :, -1].reshape(3 * depth, span_y)
    sent = jnp.concatenate([markers, other_out, x_low, x_high])
    both = lax.all_gather(sent, "col", axis=0, tiled=False)
    chip = both[:, :LIST].reshape(2 * LIST, 128)
    partner = lax.dynamic_index_in_dim(both[:, LIST:], 1 - col, 0, keepdims=False)
    plane_out = jnp.concatenate([mine_out, partner[:plane_rows]])
    partner_low = partner[plane_rows : plane_rows + 3 * depth].reshape(depth, 3, 1, span_y)
    partner_high = partner[plane_rows + 3 * depth :].reshape(depth, 3, 1, span_y)

    second = by_core(chip, gz_count, 2)
    nearest = by_core(jnp.concatenate([chip, plane_out]), gz_count, 1)
    third = by_core(second, gz_count, 1)

    slab = (gz_index * depth).astype(jnp.float32).reshape(1)
    acc = spread(markers, None, slab, dims)
    acc = spread(second, acc, slab, dims)
    acc = spread(nearest[: 2 * LIST], acc, slab, dims)
    acc = spread(third, acc, slab, dims)
    acc = acc.reshape(depth, 3, span_x, span_y)

    keep = lax.dynamic_slice_in_dim(acc, col * half_x, half_x, 2)
    give = lax.dynamic_slice_in_dim(acc, (1 - col) * half_x, half_x, 2)
    my_plane = nearest[2 * LIST : 2 * LIST + plane_rows]
    its_plane = nearest[2 * LIST + plane_rows :]
    swapped = lax.ppermute(
        jnp.concatenate([give.reshape(-1, span_y), its_plane]), "col", [(0, 1), (1, 0)]
    )
    force = keep + swapped[: depth * plane_rows].reshape(keep.shape)
    got_plane = swapped[depth * plane_rows :]
    below = jnp.where(col == 0, my_plane, got_plane).reshape(1, 3, half_x, span_y)
    above = jnp.where(col == 0, got_plane, my_plane).reshape(1, 3, half_x, span_y)
    padded = jnp.concatenate([below, velocity, above])
    across = jnp.concatenate([partner_high, velocity, partner_low], axis=2)
    neighbours = padded[2:] + padded[:-2] + across[:, :, 2:] + across[:, :, :-2]
    neighbours = neighbours + jnp.roll(velocity, 1, 3) + jnp.roll(velocity, -1, 3)
    velocity_next = velocity + viscous * (neighbours - 6.0 * velocity) + force
    return (force, velocity_next)


def solution(mesh):
    in_specs = (
        P("gz", None, "col", None),
        P(None, ("gz", "col")),
        P(None, ("gz", "col")),
        P(("gz", "col")),
        P(("gz", "col")),
        P(("gz", "col")),
        P("gz"),
    )
    out_specs = (P("gz", None, "col", None), P("gz", None, "col", None))
    return jax.shard_map(
        on_device, mesh=mesh, in_specs=in_specs, out_specs=out_specs, check_vma=False
    )
```

```python
import jax
import jax.numpy as jnp
from jax import lax
from jax.experimental import pallas as pl
from jax.experimental.pallas import tpu as pltpu
from jax.sharding import PartitionSpec as P

viscous = 0.15
ROWS = 32
ATTRS = 9
LIST = ROWS * ATTRS
KROWS = 8
SLOTS = 24
TILE = 16


def vmem():
    return pl.BlockSpec(memory_space=pltpu.VMEM)


def smem():
    return pl.BlockSpec(memory_space=pltpu.SMEM)


def corner_weights(t):
    q = jnp.sqrt(1.0 + 4.0 * t - 4.0 * t * t)
    return (
        (3.0 - 2.0 * t - q) / 8.0,
        (3.0 - 2.0 * t + q) / 8.0,
        (1.0 + 2.0 * t + q) / 8.0,
        (1.0 + 2.0 * t - q) / 8.0,
    )


def in_vmem(x):
    return pltpu.with_memory_space_constraint(x, pltpu.VMEM)


def prepare(list_ref, n, first_plane, dims, rows_ref):
    depth, span_x, span_y, span_z = dims

    def attr(a):
        return list_ref[pl.ds(n * LIST + a * ROWS, ROWS), :]

    def put(slot, value):
        rows_ref[pl.ds((n * SLOTS + slot) * ROWS, ROWS), :] = value

    def along(slot, cell, weights, span):
        tile = jnp.floor(cell * (1.0 / TILE))
        low = cell - tile * float(TILE)
        for b in range(4):
            at = low + float(b)
            put(slot + b, jnp.where(at >= float(TILE), at - float(TILE), at))
            put(slot + 4 + b, weights[b])
        put(slot + 8, tile)
        put(slot + 9, jnp.where(tile >= float(span // TILE - 1), 0.0, tile + 1.0))

    along(0, attr(6), corner_weights(attr(3)), span_x)
    rounded = [w.astype(jnp.bfloat16).astype(jnp.float32) for w in corner_weights(attr(4))]
    along(10, attr(7), rounded, span_y)
    wz = corner_weights(attr(5))
    rel = attr(8) - first_plane
    half = float(span_z // 2)
    rel = jnp.where(rel >= half, rel - float(span_z), rel)
    rel = jnp.where(rel < -half, rel + float(span_z), rel)
    for z in range(depth):
        plane = jnp.zeros_like(rel)
        for a in range(4):
            plane = jnp.where(rel == float(z - a), wz[a], plane)
        put(20 + z, plane)


def build(list_ref, rows_ref, turn, dims, a_ref, b_ref):
    depth, span_x, span_y, _ = dims
    per_list = ROWS // KROWS
    n = turn // per_list
    row = (turn % per_list) * KROWS
    row_at = lax.broadcasted_iota(jnp.int32, (TILE, 128), 0).astype(jnp.float32)
    nothing = jnp.zeros((TILE, 128), jnp.bfloat16)
    for r in range(KROWS):
        lanes = pl.ds(r * 128, 128)

        def get(slot):
            return rows_ref[pl.ds((n * SLOTS + slot) * ROWS + row + r, 1), :]

        def pattern(slot):
            weights = jnp.zeros((TILE, 128), jnp.float32)
            for b in range(4):
                weights = jnp.where(row_at == get(slot + b), get(slot + 4 + b), weights)
            tiles = jnp.where(row_at >= get(slot), get(slot + 8), get(slot + 9))
            return weights, tiles.astype(jnp.bfloat16)

        wx, x_tile = pattern(0)
        forces = [list_ref[pl.ds(n * LIST + c * ROWS + row + r, 1), :] for c in range(3)]
        a_rows = [(wx * f).astype(jnp.bfloat16) for f in forces]
        for t in range(span_x // TILE):
            here = x_tile == jnp.bfloat16(t)
            for c in range(3):
                a_ref[pl.ds(c * span_x + t * TILE, TILE), lanes] = jnp.where(here, a_rows[c], nothing)
        wy, y_tile = pattern(10)
        b_rows = [(wy * get(20 + z)).astype(jnp.bfloat16) for z in range(depth)]
        for t in range(span_y // TILE):
            here = y_tile == jnp.bfloat16(t)
            for z in range(depth):
                b_ref[pl.ds(z * span_y + t * TILE, TILE), lanes] = jnp.where(here, b_rows[z], nothing)


def spread_lists(list_ref, lists, first_plane, acc_ref, dims, rows_ref, bufs):
    depth, span_x, span_y, _ = dims
    turns = lists * (ROWS // KROWS)
    for n in range(lists):
        prepare(list_ref, n, first_plane, dims, rows_ref)

    def fill(turn, which):
        build(list_ref, rows_ref, turn, dims, *bufs[which])

    def add(which):
        a_ref, b_ref = bufs[which]
        out = lax.dot_general(
            a_ref[...], b_ref[...], (((1,), (1,)), ((), ())), preferred_element_type=jnp.float32
        )
        for z in range(depth):
            acc_ref[z] += out[:, z * span_y : (z + 1) * span_y]

    fill(0, 0)

    def two_turns(i, carry):
        fill(2 * i + 1, 1)
        add(0)
        fill(jnp.minimum(2 * i + 2, turns - 1), 0)
        add(1)
        return carry

    lax.fori_loop(0, turns // 2, two_turns, 0)


def scratch(lists, dims):
    depth, span_x, span_y, _ = dims
    a = pltpu.VMEM((3 * span_x, KROWS * 128), jnp.bfloat16)
    b = pltpu.VMEM((depth * span_y, KROWS * 128), jnp.bfloat16)
    return [pltpu.VMEM((lists * SLOTS * ROWS, 128), jnp.float32), a, b, a, b]


def cost(lists, dims):
    depth, span_x, span_y, _ = dims
    return pl.CostEstimate(
        flops=lists * ROWS * 128 * 3 * span_x * depth * span_y * 2,
        bytes_accessed=2000000,
        transcendentals=0,
    )


def spread(markers, lists, acc, plane, dims):
    depth, span_x, span_y, _ = dims

    def kernel(*refs):
        if acc is None:
            plane_ref, list_ref, out_ref, rows_ref, a0, b0, a1, b1 = refs
            out_ref[...] = jnp.zeros_like(out_ref)
        else:
            plane_ref, list_ref, _, out_ref, rows_ref, a0, b0, a1, b1 = refs
        spread_lists(list_ref, lists, plane_ref[0], out_ref, dims, rows_ref, ((a0, b0), (a1, b1)))

    operands = (plane, in_vmem(markers))
    if acc is not None:
        operands += (in_vmem(acc),)
    return pl.pallas_call(
        kernel,
        out_shape=pltpu.VMEM((depth, 3 * span_x, span_y), jnp.float32),
        in_specs=[smem()] + [vmem()] * (len(operands) - 1),
        out_specs=vmem(),
        input_output_aliases={} if acc is None else {2: 0},
        scratch_shapes=scratch(lists, dims),
        cost_estimate=cost(lists, dims),
        name="spread",
    )(*operands)


def spread_last(markers, lists, acc, nearest, plane, col, dims):
    depth, span_x, span_y, _ = dims
    half = span_x // 2
    rows = depth * 3 * half
    plane_at = 2 * LIST + 3 * half

    def kernel(plane_ref, col_ref, list_ref, in_ref, near_ref, keep_ref, give_ref, acc_ref, rows_ref, a0, b0, a1, b1):
        acc_ref[...] = in_ref[...]
        give_ref[pl.ds(rows, 3 * half), :] = near_ref[pl.ds(plane_at, 3 * half), :]
        spread_lists(list_ref, lists, plane_ref[0], acc_ref, dims, rows_ref, ((a0, b0), (a1, b1)))
        mine = pl.multiple_of(col_ref[0] * half, half)
        other = pl.multiple_of((1 - col_ref[0]) * half, half)
        for z in range(depth):
            for c in range(3):
                at = pl.ds((z * 3 + c) * half, half)
                keep_ref[at, :] = acc_ref[z, pl.ds(c * span_x + mine, half), :]
                give_ref[at, :] = acc_ref[z, pl.ds(c * span_x + other, half), :]

    return pl.pallas_call(
        kernel,
        out_shape=(
            pltpu.VMEM((rows, span_y), jnp.float32),
            pltpu.VMEM((rows + 3 * half, span_y), jnp.float32),
        ),
        in_specs=[smem(), smem(), vmem(), vmem(), vmem()],
        out_specs=(vmem(), vmem()),
        scratch_shapes=[pltpu.VMEM((depth, 3 * span_x, span_y), jnp.float32)] + scratch(lists, dims),
        cost_estimate=cost(lists, dims),
        name="spread_last",
    )(plane, col, in_vmem(markers), in_vmem(acc), in_vmem(nearest))


def pack(velocity, forces, offsets, cell_x, cell_y, cell_z, band_start, col):
    depth, _, half, span_y = velocity.shape
    plane_rows = 3 * half
    total = LIST + plane_rows + 6 * depth

    def kernel(col_ref, start_ref, v_ref, f_ref, o_ref, x_ref, y_ref, z_ref, sent_ref, plane_ref):
        for k in range(ROWS):
            for c in range(3):
                sent_ref[pl.ds(c * ROWS + k, 1), :] = f_ref[pl.ds(c, 1), pl.ds(k * 128, 128)]
                sent_ref[pl.ds((3 + c) * ROWS + k, 1), :] = o_ref[pl.ds(c, 1), pl.ds(k * 128, 128)]
        sent_ref[pl.ds(6 * ROWS, ROWS), :] = x_ref[...].astype(jnp.float32)
        sent_ref[pl.ds(7 * ROWS, ROWS), :] = y_ref[...].astype(jnp.float32)
        sent_ref[pl.ds(8 * ROWS, ROWS), :] = (z_ref[...] + start_ref[0] * depth).astype(jnp.float32)
        to_core = jnp.where(col_ref[0] == 0, 0, depth - 1)
        for c in range(3):
            sent_ref[pl.ds(LIST + c * half, half), :] = v_ref[to_core, c]
            plane_ref[pl.ds(c * half, half), :] = v_ref[depth - 1 - to_core, c]
        for z in range(depth):
            for c in range(3):
                at = LIST + plane_rows + z * 3 + c
                sent_ref[pl.ds(at, 1), :] = v_ref[z, c, pl.ds(0, 1), :]
                sent_ref[pl.ds(at + 3 * depth, 1), :] = v_ref[z, c, pl.ds(half - 1, 1), :]

    return pl.pallas_call(
        kernel,
        out_shape=(
            pltpu.VMEM((total, span_y), jnp.float32),
            pltpu.VMEM((plane_rows, span_y), jnp.float32),
        ),
        in_specs=[smem(), smem()] + [vmem()] * 6,
        out_specs=(vmem(), vmem()),
        name="pack",
    )(
        col,
        band_start,
        velocity,
        forces,
        offsets,
        cell_x.reshape(ROWS, 128),
        cell_y.reshape(ROWS, 128),
        cell_z.reshape(ROWS, 128),
    )


def by_core(x, gz_count, by):
    pairs = []
    for g in range(gz_count):
        pairs.append((2 * g, 2 * ((g + by) % gz_count)))
        pairs.append((2 * g + 1, 2 * ((g - by) % gz_count) + 1))
    return lax.ppermute(x, ("gz", "col"), pairs)


def on_device(velocity, forces, offsets, cell_x, cell_y, cell_z, band_start):
    depth, _, half_x, span_y = velocity.shape
    gz_count = lax.axis_size("gz")
    gz_index = lax.axis_index("gz")
    col = lax.axis_index("col")
    span_x = half_x * lax.axis_size("col")
    dims = (depth, span_x, span_y, gz_count * depth)
    core = col.reshape(1)
    plane_rows = 3 * half_x
    sent, mine_out = pack(velocity, forces, offsets, cell_x, cell_y, cell_z, band_start, core)
    both = lax.all_gather(sent, "col", axis=0, tiled=False)
    chip = both[:, :LIST].reshape(2 * LIST, 128)
    partner = lax.dynamic_index_in_dim(both[:, LIST:], 1 - col, 0, keepdims=False)
    plane_out = jnp.concatenate([mine_out, partner[:plane_rows]])
    partner_low = partner[plane_rows : plane_rows + 3 * depth].reshape(depth, 3, 1, span_y)
    partner_high = partner[plane_rows + 3 * depth :].reshape(depth, 3, 1, span_y)

    second = by_core(chip, gz_count, 2)
    nearest = by_core(jnp.concatenate([chip, plane_out]), gz_count, 1)
    third = by_core(second, gz_count, 1)

    slab = (gz_index * depth).astype(jnp.float32).reshape(1)
    acc = spread(sent, 1, None, slab, dims)
    acc = spread(second, 2, acc, slab, dims)
    acc = spread(nearest, 2, acc, slab, dims)
    keep, give = spread_last(third, 2, acc, nearest, slab, core, dims)
    my_plane = nearest[2 * LIST : 2 * LIST + plane_rows]
    swapped = lax.ppermute(give, "col", [(0, 1), (1, 0)])
    keep = keep.reshape(depth, 3, half_x, span_y)
    force = keep + swapped[: depth * plane_rows].reshape(keep.shape)
    got_plane = swapped[depth * plane_rows :]
    below = jnp.where(col == 0, my_plane, got_plane).reshape(1, 3, half_x, span_y)
    above = jnp.where(col == 0, got_plane, my_plane).reshape(1, 3, half_x, span_y)
    padded = jnp.concatenate([below, velocity, above])
    across = jnp.concatenate([partner_high, velocity, partner_low], axis=2)
    neighbours = padded[2:] + padded[:-2] + across[:, :, 2:] + across[:, :, :-2]
    neighbours = neighbours + jnp.roll(velocity, 1, 3) + jnp.roll(velocity, -1, 3)
    velocity_next = velocity + viscous * (neighbours - 6.0 * velocity) + force
    return (force, velocity_next)


def solution(mesh):
    in_specs = (
        P("gz", None, "col", None),
        P(None, ("gz", "col")),
        P(None, ("gz", "col")),
        P(("gz", "col")),
        P(("gz", "col")),
        P(("gz", "col")),
        P("gz"),
    )
    out_specs = (P("gz", None, "col", None), P("gz", None, "col", None))
    return jax.shard_map(
        on_device, mesh=mesh, in_specs=in_specs, out_specs=out_specs, check_vma=False
    )
```

```python
import jax
import jax.numpy as jnp
from jax import lax
from jax.experimental import pallas as pl
from jax.experimental.pallas import tpu as pltpu
from jax.sharding import PartitionSpec as P

viscous = 0.15
ROWS = 32
ATTRS = 9
LIST = ROWS * ATTRS
KROWS = 8
KERNEL_VMEM = 16 << 20
SLOTS = 24
TILE = 16


def vmem():
    return pl.BlockSpec(memory_space=pltpu.VMEM)


def smem():
    return pl.BlockSpec(memory_space=pltpu.SMEM)


def corner_weights(t):
    q = jnp.sqrt(1.0 + 4.0 * t - 4.0 * t * t)
    return (
        (3.0 - 2.0 * t - q) / 8.0,
        (3.0 - 2.0 * t + q) / 8.0,
        (1.0 + 2.0 * t + q) / 8.0,
        (1.0 + 2.0 * t - q) / 8.0,
    )


def in_vmem(x):
    return pltpu.with_memory_space_constraint(x, pltpu.VMEM)


def prepare(list_ref, n, first_plane, dims, rows_ref):
    depth, span_x, span_y, span_z = dims

    def attr(a):
        return list_ref[pl.ds(n * LIST + a * ROWS, ROWS), :]

    def put(slot, value):
        rows_ref[pl.ds((n * SLOTS + slot) * ROWS, ROWS), :] = value

    def along(slot, cell, weights, span):
        tile = jnp.floor(cell * (1.0 / TILE))
        low = cell - tile * float(TILE)
        for b in range(4):
            at = low + float(b)
            put(slot + b, jnp.where(at >= float(TILE), at - float(TILE), at))
            put(slot + 4 + b, weights[b])
        put(slot + 8, tile)
        put(slot + 9, jnp.where(tile >= float(span // TILE - 1), 0.0, tile + 1.0))

    along(0, attr(6), corner_weights(attr(3)), span_x)
    rounded = [w.astype(jnp.bfloat16).astype(jnp.float32) for w in corner_weights(attr(4))]
    along(10, attr(7), rounded, span_y)
    wz = corner_weights(attr(5))
    rel = attr(8) - first_plane
    half = float(span_z // 2)
    rel = jnp.where(rel >= half, rel - float(span_z), rel)
    rel = jnp.where(rel < -half, rel + float(span_z), rel)
    for z in range(depth):
        plane = jnp.zeros_like(rel)
        for a in range(4):
            plane = jnp.where(rel == float(z - a), wz[a], plane)
        put(20 + z, plane)


def build(list_ref, rows_ref, turn, dims, a_ref, b_ref):
    depth, span_x, span_y, _ = dims
    per_list = ROWS // KROWS
    n = turn // per_list
    row = (turn % per_list) * KROWS
    row_at = lax.broadcasted_iota(jnp.int32, (TILE, 128), 0).astype(jnp.float32)
    nothing = jnp.zeros((TILE, 128), jnp.bfloat16)
    for r in range(KROWS):
        lanes = pl.ds(r * 128, 128)

        def get(slot):
            return rows_ref[pl.ds((n * SLOTS + slot) * ROWS + row + r, 1), :]

        def pattern(slot):
            weights = jnp.zeros((TILE, 128), jnp.float32)
            for b in range(4):
                weights = jnp.where(row_at == get(slot + b), get(slot + 4 + b), weights)
            tiles = jnp.where(row_at >= get(slot), get(slot + 8), get(slot + 9))
            return weights, tiles.astype(jnp.bfloat16)

        wx, x_tile = pattern(0)
        forces = [list_ref[pl.ds(n * LIST + c * ROWS + row + r, 1), :] for c in range(3)]
        a_rows = [(wx * f).astype(jnp.bfloat16) for f in forces]
        for t in range(span_x // TILE):
            here = x_tile == jnp.bfloat16(t)
            for c in range(3):
                a_ref[pl.ds(c * span_x + t * TILE, TILE), lanes] = jnp.where(here, a_rows[c], nothing)
        wy, y_tile = pattern(10)
        b_rows = [(wy * get(20 + z)).astype(jnp.bfloat16) for z in range(depth)]
        for t in range(span_y // TILE):
            here = y_tile == jnp.bfloat16(t)
            for z in range(depth):
                b_ref[pl.ds(z * span_y + t * TILE, TILE), lanes] = jnp.where(here, b_rows[z], nothing)


def spread_lists(list_ref, lists, first_plane, acc_ref, dims, rows_ref):
    depth, span_x, span_y, _ = dims
    a = pltpu.VMEM((3 * span_x, KROWS * 128), jnp.bfloat16)
    b = pltpu.VMEM((depth * span_y, KROWS * 128), jnp.bfloat16)

    def run(a0, b0, a1, b1):
        spread_turns(list_ref, lists, first_plane, acc_ref, dims, rows_ref, ((a0, b0), (a1, b1)))

    pl.run_scoped(run, a, b, a, b)


def spread_turns(list_ref, lists, first_plane, acc_ref, dims, rows_ref, bufs):
    depth, span_x, span_y, _ = dims
    turns = lists * (ROWS // KROWS)
    for n in range(lists):
        prepare(list_ref, n, first_plane, dims, rows_ref)

    def fill(turn, which):
        build(list_ref, rows_ref, turn, dims, *bufs[which])

    def add(which):
        a_ref, b_ref = bufs[which]
        out = lax.dot_general(
            a_ref[...], b_ref[...], (((1,), (1,)), ((), ())), preferred_element_type=jnp.float32
        )
        for z in range(depth):
            acc_ref[z] += out[:, z * span_y : (z + 1) * span_y]

    fill(0, 0)

    def two_turns(i, carry):
        fill(2 * i + 1, 1)
        add(0)
        fill(jnp.minimum(2 * i + 2, turns - 1), 0)
        add(1)
        return carry

    lax.fori_loop(0, turns // 2, two_turns, 0)


def scratch(lists):
    return [pltpu.VMEM((lists * SLOTS * ROWS, 128), jnp.float32)]


def cost(lists, dims):
    depth, span_x, span_y, _ = dims
    return pl.CostEstimate(
        flops=lists * ROWS * 128 * 3 * span_x * depth * span_y * 2,
        bytes_accessed=2000000,
        transcendentals=0,
    )


def spread(markers, lists, acc, plane, dims, after=None):
    depth, span_x, span_y, _ = dims

    def kernel(*refs):
        if acc is None:
            plane_ref, list_ref, out_ref, token_ref, rows_ref = refs
            out_ref[...] = jnp.zeros_like(out_ref)
        else:
            plane_ref, list_ref, out_ref, token_ref, rows_ref = refs[:2] + refs[-3:]
        token_ref[...] = jnp.zeros_like(token_ref)
        spread_lists(list_ref, lists, plane_ref[0], out_ref, dims, rows_ref)

    operands = (plane, in_vmem(markers))
    if acc is not None:
        operands += (in_vmem(acc),)
    if after is not None:
        operands += (in_vmem(after),)
    return pl.pallas_call(
        kernel,
        out_shape=(
            pltpu.VMEM((depth, 3 * span_x, span_y), jnp.float32),
            pltpu.VMEM((8, 128), jnp.float32),
        ),
        in_specs=[smem()] + [vmem()] * (len(operands) - 1),
        out_specs=(vmem(), vmem()),
        input_output_aliases={} if acc is None else {2: 0},
        scratch_shapes=scratch(lists),
        cost_estimate=cost(lists, dims),
        compiler_params=pltpu.CompilerParams(vmem_limit_bytes=KERNEL_VMEM),
        name="spread",
    )(*operands)


def spread_last(markers, lists, acc, nearest, plane, col, dims):
    depth, span_x, span_y, _ = dims
    half = span_x // 2
    rows = depth * 3 * half
    plane_at = 2 * LIST + 3 * half

    def kernel(plane_ref, col_ref, list_ref, in_ref, near_ref, keep_ref, give_ref, acc_ref, rows_ref):
        acc_ref[...] = in_ref[...]
        give_ref[pl.ds(rows, 3 * half), :] = near_ref[pl.ds(plane_at, 3 * half), :]
        spread_lists(list_ref, lists, plane_ref[0], acc_ref, dims, rows_ref)
        mine = pl.multiple_of(col_ref[0] * half, half)
        other = pl.multiple_of((1 - col_ref[0]) * half, half)
        for z in range(depth):
            for c in range(3):
                at = pl.ds((z * 3 + c) * half, half)
                keep_ref[at, :] = acc_ref[z, pl.ds(c * span_x + mine, half), :]
                give_ref[at, :] = acc_ref[z, pl.ds(c * span_x + other, half), :]

    return pl.pallas_call(
        kernel,
        out_shape=(
            pltpu.VMEM((rows, span_y), jnp.float32),
            pltpu.VMEM((rows + 3 * half, span_y), jnp.float32),
        ),
        in_specs=[smem(), smem(), vmem(), vmem(), vmem()],
        out_specs=(vmem(), vmem()),
        scratch_shapes=[pltpu.VMEM((depth, 3 * span_x, span_y), jnp.float32)] + scratch(lists),
        cost_estimate=cost(lists, dims),
        compiler_params=pltpu.CompilerParams(vmem_limit_bytes=KERNEL_VMEM),
        name="spread_last",
    )(plane, col, in_vmem(markers), in_vmem(acc), in_vmem(nearest))


def pack(velocity, forces, offsets, cell_x, cell_y, cell_z, band_start, col):
    depth, _, half, span_y = velocity.shape
    plane_rows = 3 * half
    total = LIST + plane_rows + 6 * depth

    def kernel(col_ref, start_ref, v_ref, f_ref, o_ref, x_ref, y_ref, z_ref, sent_ref, plane_ref):
        for k in range(ROWS):
            for c in range(3):
                sent_ref[pl.ds(c * ROWS + k, 1), :] = f_ref[pl.ds(c, 1), pl.ds(k * 128, 128)]
                sent_ref[pl.ds((3 + c) * ROWS + k, 1), :] = o_ref[pl.ds(c, 1), pl.ds(k * 128, 128)]
        sent_ref[pl.ds(6 * ROWS, ROWS), :] = x_ref[...].astype(jnp.float32)
        sent_ref[pl.ds(7 * ROWS, ROWS), :] = y_ref[...].astype(jnp.float32)
        sent_ref[pl.ds(8 * ROWS, ROWS), :] = (z_ref[...] + start_ref[0] * depth).astype(jnp.float32)
        to_core = jnp.where(col_ref[0] == 0, 0, depth - 1)
        for c in range(3):
            sent_ref[pl.ds(LIST + c * half, half), :] = v_ref[to_core, c]
            plane_ref[pl.ds(c * half, half), :] = v_ref[depth - 1 - to_core, c]
        for z in range(depth):
            for c in range(3):
                at = LIST + plane_rows + z * 3 + c
                sent_ref[pl.ds(at, 1), :] = v_ref[z, c, pl.ds(0, 1), :]
                sent_ref[pl.ds(at + 3 * depth, 1), :] = v_ref[z, c, pl.ds(half - 1, 1), :]

    return pl.pallas_call(
        kernel,
        out_shape=(
            pltpu.VMEM((total, span_y), jnp.float32),
            pltpu.VMEM((plane_rows, span_y), jnp.float32),
        ),
        in_specs=[smem(), smem()] + [vmem()] * 6,
        out_specs=(vmem(), vmem()),
        name="pack",
    )(
        col,
        band_start,
        velocity,
        forces,
        offsets,
        cell_x.reshape(ROWS, 128),
        cell_y.reshape(ROWS, 128),
        cell_z.reshape(ROWS, 128),
    )


def by_core(x, gz_count, by):
    pairs = []
    for g in range(gz_count):
        pairs.append((2 * g, 2 * ((g + by) % gz_count)))
        pairs.append((2 * g + 1, 2 * ((g - by) % gz_count) + 1))
    return lax.ppermute(x, ("gz", "col"), pairs)


def on_device(velocity, forces, offsets, cell_x, cell_y, cell_z, band_start):
    depth, _, half_x, span_y = velocity.shape
    gz_count = lax.axis_size("gz")
    gz_index = lax.axis_index("gz")
    col = lax.axis_index("col")
    span_x = half_x * lax.axis_size("col")
    dims = (depth, span_x, span_y, gz_count * depth)
    core = col.reshape(1)
    plane_rows = 3 * half_x
    sent, mine_out = pack(velocity, forces, offsets, cell_x, cell_y, cell_z, band_start, core)
    both = lax.all_gather(sent, "col", axis=0, tiled=False)
    chip = both[:, :LIST].reshape(2 * LIST, 128)
    partner = lax.dynamic_index_in_dim(both[:, LIST:], 1 - col, 0, keepdims=False)
    plane_out = jnp.concatenate([mine_out, partner[:plane_rows]])
    partner_low = partner[plane_rows : plane_rows + 3 * depth].reshape(depth, 3, 1, span_y)
    partner_high = partner[plane_rows + 3 * depth :].reshape(depth, 3, 1, span_y)

    slab = (gz_index * depth).astype(jnp.float32).reshape(1)
    nearest = by_core(jnp.concatenate([chip, plane_out]), gz_count, 1)
    second = by_core(chip, gz_count, 2)
    acc, _ = spread(sent, 1, None, slab, dims)
    acc, token = spread(nearest, 2, acc, slab, dims)
    second, token = lax.optimization_barrier((second, token))
    third = by_core(second, gz_count, 1)
    acc, _ = spread(second, 2, acc, slab, dims, token)
    keep, give = spread_last(third, 2, acc, nearest, slab, core, dims)
    my_plane = nearest[2 * LIST : 2 * LIST + plane_rows]
    swapped = lax.ppermute(give, "col", [(0, 1), (1, 0)])
    keep = keep.reshape(depth, 3, half_x, span_y)
    force = keep + swapped[: depth * plane_rows].reshape(keep.shape)
    got_plane = swapped[depth * plane_rows :]
    below = jnp.where(col == 0, my_plane, got_plane).reshape(1, 3, half_x, span_y)
    above = jnp.where(col == 0, got_plane, my_plane).reshape(1, 3, half_x, span_y)
    padded = jnp.concatenate([below, velocity, above])
    across = jnp.concatenate([partner_high, velocity, partner_low], axis=2)
    neighbours = padded[2:] + padded[:-2] + across[:, :, 2:] + across[:, :, :-2]
    neighbours = neighbours + jnp.roll(velocity, 1, 3) + jnp.roll(velocity, -1, 3)
    velocity_next = velocity + viscous * (neighbours - 6.0 * velocity) + force
    return (force, velocity_next)


def solution(mesh):
    in_specs = (
        P("gz", None, "col", None),
        P(None, ("gz", "col")),
        P(None, ("gz", "col")),
        P(("gz", "col")),
        P(("gz", "col")),
        P(("gz", "col")),
        P("gz"),
    )
    out_specs = (P("gz", None, "col", None), P("gz", None, "col", None))
    return jax.shard_map(
        on_device, mesh=mesh, in_specs=in_specs, out_specs=out_specs, check_vma=False
    )
```

```python
import jax
import jax.numpy as jnp
from jax import lax
from jax.experimental import pallas as pl
from jax.experimental.pallas import tpu as pltpu
from jax.sharding import PartitionSpec as P

viscous = 0.15
ROWS = 32
ATTRS = 9
LIST = ROWS * ATTRS
KROWS = 16
KERNEL_VMEM = 16 << 20
SLOTS = 24
TILE = 16


def vmem():
    return pl.BlockSpec(memory_space=pltpu.VMEM)


def smem():
    return pl.BlockSpec(memory_space=pltpu.SMEM)


def corner_weights(t):
    q = jnp.sqrt(1.0 + 4.0 * t - 4.0 * t * t)
    return (
        (3.0 - 2.0 * t - q) / 8.0,
        (3.0 - 2.0 * t + q) / 8.0,
        (1.0 + 2.0 * t + q) / 8.0,
        (1.0 + 2.0 * t - q) / 8.0,
    )


def in_vmem(x):
    return pltpu.with_memory_space_constraint(x, pltpu.VMEM)


def from_plane(list_ref, n, first_plane, span_z):
    rel = list_ref[pl.ds(n * LIST + 8 * ROWS, ROWS), :] - first_plane
    half = float(span_z // 2)
    rel = jnp.where(rel >= half, rel - float(span_z), rel)
    return jnp.where(rel < -half, rel + float(span_z), rel)


def prepare(list_ref, n, first_plane, dims, rows_ref):
    depth, span_x, span_y, span_z = dims

    def attr(a):
        return list_ref[pl.ds(n * LIST + a * ROWS, ROWS), :]

    def put(slot, value):
        rows_ref[pl.ds((n * SLOTS + slot) * ROWS, ROWS), :] = value

    def along(slot, cell, weights, span):
        tile = jnp.floor(cell * (1.0 / TILE))
        low = cell - tile * float(TILE)
        for b in range(4):
            at = low + float(b)
            put(slot + b, jnp.where(at >= float(TILE), at - float(TILE), at))
            put(slot + 4 + b, weights[b])
        put(slot + 8, tile)
        put(slot + 9, jnp.where(tile >= float(span // TILE - 1), 0.0, tile + 1.0))

    along(0, attr(6), corner_weights(attr(3)), span_x)
    rounded = [w.astype(jnp.bfloat16).astype(jnp.float32) for w in corner_weights(attr(4))]
    along(10, attr(7), rounded, span_y)
    wz = corner_weights(attr(5))
    rel = from_plane(list_ref, n, first_plane, span_z)
    for z in range(depth):
        plane = jnp.zeros_like(rel)
        for a in range(4):
            plane = jnp.where(rel == float(z - a), wz[a], plane)
        put(20 + z, plane)


def build(list_ref, rows_ref, turn, dims, a_ref, b_ref):
    depth, span_x, span_y, _ = dims
    per_list = ROWS // KROWS
    n = turn // per_list
    row = (turn % per_list) * KROWS
    row_at = lax.broadcasted_iota(jnp.int32, (TILE, 128), 0).astype(jnp.float32)
    nothing = jnp.zeros((TILE, 128), jnp.bfloat16)
    for r in range(KROWS):
        lanes = pl.ds(r * 128, 128)

        def get(slot):
            return rows_ref[pl.ds((n * SLOTS + slot) * ROWS + row + r, 1), :]

        def pattern(slot):
            weights = jnp.zeros((TILE, 128), jnp.float32)
            for b in range(4):
                weights = jnp.where(row_at == get(slot + b), get(slot + 4 + b), weights)
            tiles = jnp.where(row_at >= get(slot), get(slot + 8), get(slot + 9))
            return weights, tiles.astype(jnp.bfloat16)

        wx, x_tile = pattern(0)
        forces = [list_ref[pl.ds(n * LIST + c * ROWS + row + r, 1), :] for c in range(3)]
        a_rows = [(wx * f).astype(jnp.bfloat16) for f in forces]
        for t in range(span_x // TILE):
            here = x_tile == jnp.bfloat16(t)
            for c in range(3):
                a_ref[pl.ds(c * span_x + t * TILE, TILE), lanes] = jnp.where(here, a_rows[c], nothing)
        wy, y_tile = pattern(10)
        b_rows = [(wy * get(20 + z)).astype(jnp.bfloat16) for z in range(depth)]
        for t in range(span_y // TILE):
            here = y_tile == jnp.bfloat16(t)
            for z in range(depth):
                b_ref[pl.ds(z * span_y + t * TILE, TILE), lanes] = jnp.where(here, b_rows[z], nothing)


def spread_lists(list_ref, lists, first_plane, acc_ref, dims, rows_ref):
    depth, span_x, span_y, _ = dims
    a = pltpu.VMEM((3 * span_x, KROWS * 128), jnp.bfloat16)
    b = pltpu.VMEM((depth * span_y, KROWS * 128), jnp.bfloat16)

    def run(a0, b0, a1, b1):
        spread_turns(list_ref, lists, first_plane, acc_ref, dims, rows_ref, ((a0, b0), (a1, b1)))

    touch = jnp.zeros((ROWS, 128), jnp.float32)
    for n in range(lists):
        rel = from_plane(list_ref, n, first_plane, dims[3])
        touch = jnp.where(jnp.logical_and(rel > -4.0, rel < float(depth)), 1.0, touch)

    @pl.when(jnp.max(touch) > 0.0)
    def _():
        pl.run_scoped(run, a, b, a, b)


def spread_turns(list_ref, lists, first_plane, acc_ref, dims, rows_ref, bufs):
    depth, span_x, span_y, _ = dims
    turns = lists * (ROWS // KROWS)
    for n in range(lists):
        prepare(list_ref, n, first_plane, dims, rows_ref)

    def fill(turn, which):
        build(list_ref, rows_ref, turn, dims, *bufs[which])

    def add(which):
        a_ref, b_ref = bufs[which]
        out = lax.dot_general(
            a_ref[...], b_ref[...], (((1,), (1,)), ((), ())), preferred_element_type=jnp.float32
        )
        for z in range(depth):
            acc_ref[z] += out[:, z * span_y : (z + 1) * span_y]

    fill(0, 0)

    def two_turns(i, carry):
        fill(2 * i + 1, 1)
        add(0)
        fill(jnp.minimum(2 * i + 2, turns - 1), 0)
        add(1)
        return carry

    lax.fori_loop(0, turns // 2, two_turns, 0)


def scratch(lists):
    return [pltpu.VMEM((lists * SLOTS * ROWS, 128), jnp.float32)]


def cost(lists, dims):
    depth, span_x, span_y, _ = dims
    return pl.CostEstimate(
        flops=lists * ROWS * 128 * 3 * span_x * depth * span_y * 2,
        bytes_accessed=2000000,
        transcendentals=0,
    )


def own_plane(depth):
    return (lax.axis_index("gz") * depth).astype(jnp.float32)


def spread(markers, lists, acc, dims):
    depth, span_x, span_y, _ = dims

    def kernel(*refs):
        if acc is None:
            list_ref, out_ref, rows_ref = refs
            out_ref[...] = jnp.zeros_like(out_ref)
        else:
            list_ref, _, out_ref, rows_ref = refs
        spread_lists(list_ref, lists, own_plane(depth), out_ref, dims, rows_ref)

    operands = (in_vmem(markers),)
    if acc is not None:
        operands += (in_vmem(acc),)
    return pl.pallas_call(
        kernel,
        out_shape=pltpu.VMEM((depth, 3 * span_x, span_y), jnp.float32),
        in_specs=[vmem()] * len(operands),
        out_specs=vmem(),
        input_output_aliases={} if acc is None else {1: 0},
        scratch_shapes=scratch(lists),
        cost_estimate=cost(lists, dims),
        compiler_params=pltpu.CompilerParams(vmem_limit_bytes=KERNEL_VMEM),
        name="spread",
    )(*operands)


def spread_last(markers, lists, acc, planes, planes_at, dims):
    depth, span_x, span_y, _ = dims
    half = span_x // 2
    rows = depth * 3 * half

    def kernel(list_ref, in_ref, planes_ref, keep_ref, give_ref, acc_ref, rows_ref):
        acc_ref[...] = in_ref[...]
        give_ref[pl.ds(rows, 3 * half), :] = planes_ref[pl.ds(planes_at + 3 * half, 3 * half), :]
        spread_lists(list_ref, lists, own_plane(depth), acc_ref, dims, rows_ref)
        col = lax.axis_index("col")
        mine = pl.multiple_of(col * half, half)
        other = pl.multiple_of((1 - col) * half, half)
        for z in range(depth):
            for c in range(3):
                at = pl.ds((z * 3 + c) * half, half)
                keep_ref[at, :] = acc_ref[z, pl.ds(c * span_x + mine, half), :]
                give_ref[at, :] = acc_ref[z, pl.ds(c * span_x + other, half), :]

    return pl.pallas_call(
        kernel,
        out_shape=(
            pltpu.VMEM((rows, span_y), jnp.float32),
            pltpu.VMEM((rows + 3 * half, span_y), jnp.float32),
        ),
        in_specs=[vmem(), vmem(), vmem()],
        out_specs=(vmem(), vmem()),
        scratch_shapes=[pltpu.VMEM((depth, 3 * span_x, span_y), jnp.float32)] + scratch(lists),
        cost_estimate=cost(lists, dims),
        compiler_params=pltpu.CompilerParams(vmem_limit_bytes=KERNEL_VMEM),
        name="spread_last",
    )(in_vmem(markers), in_vmem(acc), in_vmem(planes))


def viscous_part(velocity, both, planes, planes_at):
    depth, _, half, span_y = velocity.shape
    low_at = LIST + 3 * half

    def kernel(v_ref, both_ref, planes_ref, base_ref):
        col = lax.axis_index("col")
        row_at = lax.broadcasted_iota(jnp.int32, (half, span_y), 0)
        for z in range(depth):
            for c in range(3):
                v = v_ref[z, c]
                x_low = both_ref[1 - col, pl.ds(low_at + z * 3 + c, 1), :]
                x_high = both_ref[1 - col, pl.ds(low_at + 3 * depth + z * 3 + c, 1), :]
                near = jnp.where(row_at == 0, x_high, pltpu.roll(v, 1, 0))
                near = near + jnp.where(row_at == half - 1, x_low, pltpu.roll(v, half - 1, 0))
                near = near + pltpu.roll(v, 1, 1) + pltpu.roll(v, span_y - 1, 1)
                if z > 0:
                    near = near + v_ref[z - 1, c]
                if z < depth - 1:
                    near = near + v_ref[z + 1, c]
                base_ref[z, c] = v + viscous * (near - 6.0 * v)
        at = jnp.where(col == 0, 0, depth - 1)
        for c in range(3):
            base_ref[at, c] += viscous * planes_ref[pl.ds(planes_at + c * half, half), :]

    return pl.pallas_call(
        kernel,
        out_shape=pltpu.VMEM(velocity.shape, jnp.float32),
        in_specs=[vmem(), vmem(), vmem()],
        out_specs=vmem(),
        cost_estimate=pl.CostEstimate(flops=4000000, bytes_accessed=2000000, transcendentals=0),
        compiler_params=pltpu.CompilerParams(vmem_limit_bytes=KERNEL_VMEM),
        name="viscous_part",
    )(in_vmem(velocity), in_vmem(both), in_vmem(planes))


def finish(keep, swapped, base):
    depth, _, half, span_y = base.shape
    rows = depth * 3 * half

    def kernel(keep_ref, swap_ref, base_ref, force_hbm, next_hbm, force_ref, next_ref, sems):
        col = lax.axis_index("col")
        at = jnp.where(col == 0, depth - 1, 0)
        copies = []
        for z in range(depth):
            share = jnp.where(at == z, viscous, 0.0)
            for c in range(3):
                here = pl.ds((z * 3 + c) * half, half)
                force = keep_ref[here, :] + swap_ref[here, :]
                force_ref[z, c] = force
                plane = swap_ref[pl.ds(rows + c * half, half), :]
                next_ref[z, c] = base_ref[z, c] + force + share * plane
            copies.append(pltpu.make_async_copy(force_ref.at[z], force_hbm.at[z], sems.at[0, z]))
            copies.append(pltpu.make_async_copy(next_ref.at[z], next_hbm.at[z], sems.at[1, z]))
            copies[-2].start()
            copies[-1].start()
        for copy in copies:
            copy.wait()

    out = jax.ShapeDtypeStruct(base.shape, jnp.float32)
    return pl.pallas_call(
        kernel,
        out_shape=(out, out),
        in_specs=[vmem(), vmem(), vmem()],
        out_specs=(pl.BlockSpec(memory_space=pl.ANY), pl.BlockSpec(memory_space=pl.ANY)),
        scratch_shapes=[
            pltpu.VMEM(base.shape, jnp.float32),
            pltpu.VMEM(base.shape, jnp.float32),
            pltpu.SemaphoreType.DMA((2, depth)),
        ],
        compiler_params=pltpu.CompilerParams(vmem_limit_bytes=KERNEL_VMEM),
        name="finish",
    )(in_vmem(keep), in_vmem(swapped), in_vmem(base))


def pack(velocity, forces, offsets, cell_x, cell_y, cell_z, band_start):
    depth, _, half, span_y = velocity.shape
    plane_rows = 3 * half
    total = LIST + plane_rows + 6 * depth

    def kernel(start_ref, v_ref, f_ref, o_ref, x_ref, y_ref, z_ref, sent_ref, plane_ref):
        for k in range(ROWS):
            for c in range(3):
                sent_ref[pl.ds(c * ROWS + k, 1), :] = f_ref[pl.ds(c, 1), pl.ds(k * 128, 128)]
                sent_ref[pl.ds((3 + c) * ROWS + k, 1), :] = o_ref[pl.ds(c, 1), pl.ds(k * 128, 128)]
        sent_ref[pl.ds(6 * ROWS, ROWS), :] = x_ref[...].astype(jnp.float32)
        sent_ref[pl.ds(7 * ROWS, ROWS), :] = y_ref[...].astype(jnp.float32)
        sent_ref[pl.ds(8 * ROWS, ROWS), :] = (z_ref[...] + start_ref[0] * depth).astype(jnp.float32)
        to_core = jnp.where(lax.axis_index("col") == 0, 0, depth - 1)
        for c in range(3):
            sent_ref[pl.ds(LIST + c * half, half), :] = v_ref[to_core, c]
            plane_ref[pl.ds(c * half, half), :] = v_ref[depth - 1 - to_core, c]
        for z in range(depth):
            for c in range(3):
                at = LIST + plane_rows + z * 3 + c
                sent_ref[pl.ds(at, 1), :] = v_ref[z, c, pl.ds(0, 1), :]
                sent_ref[pl.ds(at + 3 * depth, 1), :] = v_ref[z, c, pl.ds(half - 1, 1), :]

    return pl.pallas_call(
        kernel,
        out_shape=(
            pltpu.VMEM((total, span_y), jnp.float32),
            pltpu.VMEM((plane_rows, span_y), jnp.float32),
        ),
        in_specs=[smem()] + [vmem()] * 6,
        out_specs=(vmem(), vmem()),
        name="pack",
    )(
        band_start,
        velocity,
        forces,
        offsets,
        cell_x.reshape(ROWS, 128),
        cell_y.reshape(ROWS, 128),
        cell_z.reshape(ROWS, 128),
    )


def by_core(x, gz_count, by):
    pairs = []
    for g in range(gz_count):
        pairs.append((2 * g, 2 * ((g + by) % gz_count)))
        pairs.append((2 * g + 1, 2 * ((g - by) % gz_count) + 1))
    return lax.ppermute(x, ("gz", "col"), pairs)


def on_device(velocity, forces, offsets, cell_x, cell_y, cell_z, band_start):
    depth, _, half_x, span_y = velocity.shape
    gz_count = lax.axis_size("gz")
    col = lax.axis_index("col")
    span_x = half_x * lax.axis_size("col")
    dims = (depth, span_x, span_y, gz_count * depth)
    plane_rows = 3 * half_x
    sent, mine_out = pack(velocity, forces, offsets, cell_x, cell_y, cell_z, band_start)
    both = lax.all_gather(sent, "col", axis=0, tiled=False)
    chip = both[:, :LIST].reshape(2 * LIST, 128)
    partner = lax.dynamic_index_in_dim(both[:, LIST : LIST + plane_rows], 1 - col, 0, keepdims=False)

    second = by_core(chip, gz_count, 2)
    nearest = by_core(jnp.concatenate([chip, mine_out, partner]), gz_count, 1)
    acc = spread(sent, 1, None, dims)
    third = by_core(second, gz_count, 1)
    acc = spread(second, 2, acc, dims)
    acc = spread(nearest, 2, acc, dims)
    keep, give = spread_last(third, 2, acc, nearest, 2 * LIST, dims)
    swapped = lax.ppermute(give, "col", [(0, 1), (1, 0)])
    base = viscous_part(velocity, both, nearest, 2 * LIST)
    return finish(keep, swapped, base)


def solution(mesh):
    in_specs = (
        P("gz", None, "col", None),
        P(None, ("gz", "col")),
        P(None, ("gz", "col")),
        P(("gz", "col")),
        P(("gz", "col")),
        P(("gz", "col")),
        P("gz"),
    )
    out_specs = (P("gz", None, "col", None), P("gz", None, "col", None))
    return jax.shard_map(
        on_device, mesh=mesh, in_specs=in_specs, out_specs=out_specs, check_vma=False
    )
```

```python
import jax
import jax.numpy as jnp
from jax import lax
from jax.experimental import pallas as pl
from jax.experimental.pallas import tpu as pltpu
from jax.sharding import PartitionSpec as P

viscous = 0.15
ROWS = 32
ATTRS = 9
LIST = ROWS * ATTRS
KROWS = 16
KERNEL_VMEM = 16 << 20
SLOTS = 24
TILE = 16


def vmem():
    return pl.BlockSpec(memory_space=pltpu.VMEM)


def smem():
    return pl.BlockSpec(memory_space=pltpu.SMEM)


def corner_weights(t):
    q = jnp.sqrt(1.0 + 4.0 * t - 4.0 * t * t)
    return (
        (3.0 - 2.0 * t - q) / 8.0,
        (3.0 - 2.0 * t + q) / 8.0,
        (1.0 + 2.0 * t + q) / 8.0,
        (1.0 + 2.0 * t - q) / 8.0,
    )


def in_vmem(x):
    return pltpu.with_memory_space_constraint(x, pltpu.VMEM)


def from_plane(list_ref, n, first_plane, span_z):
    rel = list_ref[pl.ds(n * LIST + 8 * ROWS, ROWS), :] - first_plane
    half = float(span_z // 2)
    rel = jnp.where(rel >= half, rel - float(span_z), rel)
    return jnp.where(rel < -half, rel + float(span_z), rel)


def prepare(list_ref, n, first_plane, dims, rows_ref):
    depth, span_x, span_y, span_z = dims

    def attr(a):
        return list_ref[pl.ds(n * LIST + a * ROWS, ROWS), :]

    def put(slot, value):
        rows_ref[pl.ds((n * SLOTS + slot) * ROWS, ROWS), :] = value

    def along(slot, cell, weights, span):
        tile = jnp.floor(cell * (1.0 / TILE))
        low = cell - tile * float(TILE)
        for b in range(4):
            at = low + float(b)
            put(slot + b, jnp.where(at >= float(TILE), at - float(TILE), at))
            put(slot + 4 + b, weights[b])
        put(slot + 8, tile)
        put(slot + 9, jnp.where(tile >= float(span // TILE - 1), 0.0, tile + 1.0))

    along(0, attr(6), corner_weights(attr(3)), span_x)
    rounded = [w.astype(jnp.bfloat16).astype(jnp.float32) for w in corner_weights(attr(4))]
    along(10, attr(7), rounded, span_y)
    wz = corner_weights(attr(5))
    rel = from_plane(list_ref, n, first_plane, span_z)
    for z in range(depth):
        plane = jnp.zeros_like(rel)
        for a in range(4):
            plane = jnp.where(rel == float(z - a), wz[a], plane)
        put(20 + z, plane)


def build(list_ref, rows_ref, turn, dims, a_ref, b_ref):
    depth, span_x, span_y, _ = dims
    per_list = ROWS // KROWS
    n = turn // per_list
    row = (turn % per_list) * KROWS
    row_at = lax.broadcasted_iota(jnp.int32, (TILE, 128), 0).astype(jnp.float32)
    nothing = jnp.zeros((TILE, 128), jnp.bfloat16)
    for r in range(KROWS):
        lanes = pl.ds(r * 128, 128)

        def get(slot):
            return rows_ref[pl.ds((n * SLOTS + slot) * ROWS + row + r, 1), :]

        def pattern(slot):
            weights = jnp.zeros((TILE, 128), jnp.float32)
            for b in range(4):
                weights = jnp.where(row_at == get(slot + b), get(slot + 4 + b), weights)
            tiles = jnp.where(row_at >= get(slot), get(slot + 8), get(slot + 9))
            return weights, tiles.astype(jnp.bfloat16)

        wx, x_tile = pattern(0)
        forces = [list_ref[pl.ds(n * LIST + c * ROWS + row + r, 1), :] for c in range(3)]
        a_rows = [(wx * f).astype(jnp.bfloat16) for f in forces]
        for t in range(span_x // TILE):
            here = x_tile == jnp.bfloat16(t)
            for c in range(3):
                a_ref[pl.ds(c * span_x + t * TILE, TILE), lanes] = jnp.where(here, a_rows[c], nothing)
        wy, y_tile = pattern(10)
        b_rows = [(wy * get(20 + z)).astype(jnp.bfloat16) for z in range(depth)]
        for t in range(span_y // TILE):
            here = y_tile == jnp.bfloat16(t)
            for z in range(depth):
                b_ref[pl.ds(z * span_y + t * TILE, TILE), lanes] = jnp.where(here, b_rows[z], nothing)


def spread_lists(list_ref, lists, first_plane, acc_ref, dims, rows_ref):
    depth, span_x, span_y, _ = dims
    a = pltpu.VMEM((3 * span_x, KROWS * 128), jnp.bfloat16)
    b = pltpu.VMEM((depth * span_y, KROWS * 128), jnp.bfloat16)

    def run(a0, b0, a1, b1):
        spread_turns(list_ref, lists, first_plane, acc_ref, dims, rows_ref, ((a0, b0), (a1, b1)))

    touch = jnp.zeros((ROWS, 128), jnp.float32)
    for n in range(lists):
        rel = from_plane(list_ref, n, first_plane, dims[3])
        touch = jnp.where(jnp.logical_and(rel > -4.0, rel < float(depth)), 1.0, touch)

    @pl.when(jnp.max(touch) > 0.0)
    def _():
        pl.run_scoped(run, a, b, a, b)


def spread_turns(list_ref, lists, first_plane, acc_ref, dims, rows_ref, bufs):
    depth, span_x, span_y, _ = dims
    turns = lists * (ROWS // KROWS)
    for n in range(lists):
        prepare(list_ref, n, first_plane, dims, rows_ref)

    def fill(turn, which):
        build(list_ref, rows_ref, turn, dims, *bufs[which])

    def add(which):
        a_ref, b_ref = bufs[which]
        out = lax.dot_general(
            a_ref[...], b_ref[...], (((1,), (1,)), ((), ())), preferred_element_type=jnp.float32
        )
        for z in range(depth):
            acc_ref[z] += out[:, z * span_y : (z + 1) * span_y]

    fill(0, 0)

    def two_turns(i, carry):
        fill(2 * i + 1, 1)
        add(0)
        fill(jnp.minimum(2 * i + 2, turns - 1), 0)
        add(1)
        return carry

    lax.fori_loop(0, turns // 2, two_turns, 0)


def scratch(lists):
    return [pltpu.VMEM((lists * SLOTS * ROWS, 128), jnp.float32)]


def cost(lists, dims):
    depth, span_x, span_y, _ = dims
    return pl.CostEstimate(
        flops=lists * ROWS * 128 * 3 * span_x * depth * span_y * 2,
        bytes_accessed=2000000,
        transcendentals=0,
    )


def own_plane(depth):
    return (lax.axis_index("gz") * depth).astype(jnp.float32)


def spread(markers, lists, acc, dims):
    depth, span_x, span_y, _ = dims

    def kernel(*refs):
        if acc is None:
            list_ref, out_ref, rows_ref = refs
            out_ref[...] = jnp.zeros_like(out_ref)
        else:
            list_ref, _, out_ref, rows_ref = refs
        spread_lists(list_ref, lists, own_plane(depth), out_ref, dims, rows_ref)

    operands = (in_vmem(markers),)
    if acc is not None:
        operands += (in_vmem(acc),)
    return pl.pallas_call(
        kernel,
        out_shape=pltpu.VMEM((depth, 3 * span_x, span_y), jnp.float32),
        in_specs=[vmem()] * len(operands),
        out_specs=vmem(),
        input_output_aliases={} if acc is None else {1: 0},
        scratch_shapes=scratch(lists),
        cost_estimate=cost(lists, dims),
        compiler_params=pltpu.CompilerParams(vmem_limit_bytes=KERNEL_VMEM),
        name="spread",
    )(*operands)


def spread_last(markers, lists, acc, planes, planes_at, dims):
    depth, span_x, span_y, _ = dims
    half = span_x // 2
    rows = depth * 3 * half

    def kernel(list_ref, in_ref, planes_ref, keep_ref, give_ref, acc_ref, rows_ref):
        acc_ref[...] = in_ref[...]
        give_ref[pl.ds(rows, 3 * half), :] = planes_ref[pl.ds(planes_at + 3 * half, 3 * half), :]
        spread_lists(list_ref, lists, own_plane(depth), acc_ref, dims, rows_ref)
        col = lax.axis_index("col")
        mine = pl.multiple_of(col * half, half)
        other = pl.multiple_of((1 - col) * half, half)
        for z in range(depth):
            for c in range(3):
                at = pl.ds((z * 3 + c) * half, half)
                keep_ref[at, :] = acc_ref[z, pl.ds(c * span_x + mine, half), :]
                give_ref[at, :] = acc_ref[z, pl.ds(c * span_x + other, half), :]

    return pl.pallas_call(
        kernel,
        out_shape=(
            pltpu.VMEM((rows, span_y), jnp.float32),
            pltpu.VMEM((rows + 3 * half, span_y), jnp.float32),
        ),
        in_specs=[vmem(), vmem(), vmem()],
        out_specs=(vmem(), vmem()),
        scratch_shapes=[pltpu.VMEM((depth, 3 * span_x, span_y), jnp.float32)] + scratch(lists),
        cost_estimate=cost(lists, dims),
        compiler_params=pltpu.CompilerParams(vmem_limit_bytes=KERNEL_VMEM),
        name="spread_last",
    )(in_vmem(markers), in_vmem(acc), in_vmem(planes))


def viscous_part(velocity, both):
    depth, _, half, span_y = velocity.shape
    low_at = LIST + 3 * half

    def kernel(v_ref, both_ref, base_ref):
        col = lax.axis_index("col")
        row_at = lax.broadcasted_iota(jnp.int32, (half, span_y), 0)
        for z in range(depth):
            for c in range(3):
                v = v_ref[z, c]
                x_low = both_ref[1 - col, pl.ds(low_at + z * 3 + c, 1), :]
                x_high = both_ref[1 - col, pl.ds(low_at + 3 * depth + z * 3 + c, 1), :]
                near = jnp.where(row_at == 0, x_high, pltpu.roll(v, 1, 0))
                near = near + jnp.where(row_at == half - 1, x_low, pltpu.roll(v, half - 1, 0))
                near = near + pltpu.roll(v, 1, 1) + pltpu.roll(v, span_y - 1, 1)
                if z > 0:
                    near = near + v_ref[z - 1, c]
                if z < depth - 1:
                    near = near + v_ref[z + 1, c]
                base_ref[z, c] = v + viscous * (near - 6.0 * v)

    return pl.pallas_call(
        kernel,
        out_shape=pltpu.VMEM(velocity.shape, jnp.float32),
        in_specs=[vmem(), vmem()],
        out_specs=vmem(),
        cost_estimate=pl.CostEstimate(flops=4000000, bytes_accessed=2000000, transcendentals=0),
        compiler_params=pltpu.CompilerParams(vmem_limit_bytes=KERNEL_VMEM),
        name="viscous_part",
    )(in_vmem(velocity), in_vmem(both))


def finish(keep, given, base, planes, planes_at):
    depth, _, half, span_y = base.shape
    rows = depth * 3 * half

    def kernel(keep_ref, given_ref, base_ref, planes_ref, force_hbm, next_hbm, force_ref, next_ref, sems):
        col = lax.axis_index("col")
        mine_at = jnp.where(col == 0, 0, depth - 1)
        copies = []
        for z in range(depth):
            mine = jnp.where(mine_at == z, viscous, 0.0)
            other = jnp.where(depth - 1 - mine_at == z, viscous, 0.0)
            for c in range(3):
                here = pl.ds((z * 3 + c) * half, half)
                force = keep_ref[here, :] + given_ref[1 - col, here, :]
                force_ref[z, c] = force
                base = base_ref[z, c]
                if z == 0 or z == depth - 1:
                    base = base + mine * planes_ref[pl.ds(planes_at + c * half, half), :]
                    base = base + other * given_ref[1 - col, pl.ds(rows + c * half, half), :]
                next_ref[z, c] = base + force
            copies.append(pltpu.make_async_copy(force_ref.at[z], force_hbm.at[z], sems.at[0, z]))
            copies.append(pltpu.make_async_copy(next_ref.at[z], next_hbm.at[z], sems.at[1, z]))
            copies[-2].start()
            copies[-1].start()
        for copy in copies:
            copy.wait()

    out = jax.ShapeDtypeStruct(base.shape, jnp.float32)
    return pl.pallas_call(
        kernel,
        out_shape=(out, out),
        in_specs=[vmem()] * 4,
        out_specs=(pl.BlockSpec(memory_space=pl.ANY), pl.BlockSpec(memory_space=pl.ANY)),
        scratch_shapes=[
            pltpu.VMEM(base.shape, jnp.float32),
            pltpu.VMEM(base.shape, jnp.float32),
            pltpu.SemaphoreType.DMA((2, depth)),
        ],
        compiler_params=pltpu.CompilerParams(vmem_limit_bytes=KERNEL_VMEM),
        name="finish",
    )(in_vmem(keep), in_vmem(given), in_vmem(base), in_vmem(planes))


def pack(velocity, forces, offsets, cell_x, cell_y, cell_z, band_start):
    depth, _, half, span_y = velocity.shape
    plane_rows = 3 * half
    total = LIST + plane_rows + 6 * depth

    def kernel(start_ref, v_ref, f_ref, o_ref, x_ref, y_ref, z_ref, sent_ref, plane_ref):
        for k in range(ROWS):
            for c in range(3):
                sent_ref[pl.ds(c * ROWS + k, 1), :] = f_ref[pl.ds(c, 1), pl.ds(k * 128, 128)]
                sent_ref[pl.ds((3 + c) * ROWS + k, 1), :] = o_ref[pl.ds(c, 1), pl.ds(k * 128, 128)]
        sent_ref[pl.ds(6 * ROWS, ROWS), :] = x_ref[...].astype(jnp.float32)
        sent_ref[pl.ds(7 * ROWS, ROWS), :] = y_ref[...].astype(jnp.float32)
        sent_ref[pl.ds(8 * ROWS, ROWS), :] = (z_ref[...] + start_ref[0] * depth).astype(jnp.float32)
        to_core = jnp.where(lax.axis_index("col") == 0, 0, depth - 1)
        for c in range(3):
            sent_ref[pl.ds(LIST + c * half, half), :] = v_ref[to_core, c]
            plane_ref[pl.ds(c * half, half), :] = v_ref[depth - 1 - to_core, c]
        for z in range(depth):
            for c in range(3):
                at = LIST + plane_rows + z * 3 + c
                sent_ref[pl.ds(at, 1), :] = v_ref[z, c, pl.ds(0, 1), :]
                sent_ref[pl.ds(at + 3 * depth, 1), :] = v_ref[z, c, pl.ds(half - 1, 1), :]

    return pl.pallas_call(
        kernel,
        out_shape=(
            pltpu.VMEM((total, span_y), jnp.float32),
            pltpu.VMEM((plane_rows, span_y), jnp.float32),
        ),
        in_specs=[smem()] + [vmem()] * 6,
        out_specs=(vmem(), vmem()),
        name="pack",
    )(
        band_start,
        velocity,
        forces,
        offsets,
        cell_x.reshape(ROWS, 128),
        cell_y.reshape(ROWS, 128),
        cell_z.reshape(ROWS, 128),
    )


def by_core(x, gz_count, by):
    pairs = []
    for g in range(gz_count):
        pairs.append((2 * g, 2 * ((g + by) % gz_count)))
        pairs.append((2 * g + 1, 2 * ((g - by) % gz_count) + 1))
    return lax.ppermute(x, ("gz", "col"), pairs)


def on_device(velocity, forces, offsets, cell_x, cell_y, cell_z, band_start):
    depth, _, half_x, span_y = velocity.shape
    gz_count = lax.axis_size("gz")
    col = lax.axis_index("col")
    span_x = half_x * lax.axis_size("col")
    dims = (depth, span_x, span_y, gz_count * depth)
    plane_rows = 3 * half_x
    sent, mine_out = pack(velocity, forces, offsets, cell_x, cell_y, cell_z, band_start)
    both = lax.all_gather(sent, "col", axis=0, tiled=False)
    chip = both[:, :LIST].reshape(2 * LIST, 128)
    partner = lax.dynamic_index_in_dim(both[:, LIST : LIST + plane_rows], 1 - col, 0, keepdims=False)

    second = by_core(chip, gz_count, 2)
    nearest = by_core(jnp.concatenate([chip, mine_out, partner]), gz_count, 1)
    acc = spread(sent, 1, None, dims)
    third = by_core(second, gz_count, 1)
    acc = spread(second, 2, acc, dims)
    acc = spread(nearest, 2, acc, dims)
    keep, give = spread_last(third, 2, acc, nearest, 2 * LIST, dims)
    given = lax.all_gather(give, "col", axis=0, tiled=False)
    base = viscous_part(velocity, both)
    return finish(keep, given, base, nearest, 2 * LIST)


def solution(mesh):
    in_specs = (
        P("gz", None, "col", None),
        P(None, ("gz", "col")),
        P(None, ("gz", "col")),
        P(("gz", "col")),
        P(("gz", "col")),
        P(("gz", "col")),
        P("gz"),
    )
    out_specs = (P("gz", None, "col", None), P("gz", None, "col", None))
    return jax.shard_map(
        on_device, mesh=mesh, in_specs=in_specs, out_specs=out_specs, check_vma=False
    )
```

```python
import jax
import jax.numpy as jnp
from jax import lax
from jax.experimental import pallas as pl
from jax.experimental.pallas import tpu as pltpu
from jax.sharding import PartitionSpec as P

viscous = 0.15
ROWS = 32
ATTRS = 9
LIST = ROWS * ATTRS
KROWS = 8
KERNEL_VMEM = 16 << 20
UNROLL = 4
SLOTS = 24
TILE = 16


def vmem():
    return pl.BlockSpec(memory_space=pltpu.VMEM)


def smem():
    return pl.BlockSpec(memory_space=pltpu.SMEM)


def corner_weights(t):
    q = jnp.sqrt(1.0 + 4.0 * t - 4.0 * t * t)
    return (
        (3.0 - 2.0 * t - q) / 8.0,
        (3.0 - 2.0 * t + q) / 8.0,
        (1.0 + 2.0 * t + q) / 8.0,
        (1.0 + 2.0 * t - q) / 8.0,
    )


def in_vmem(x):
    return pltpu.with_memory_space_constraint(x, pltpu.VMEM)


def from_plane(list_ref, n, first_plane, span_z):
    rel = list_ref[pl.ds(n * LIST + 8 * ROWS, ROWS), :] - first_plane
    half = float(span_z // 2)
    rel = jnp.where(rel >= half, rel - float(span_z), rel)
    return jnp.where(rel < -half, rel + float(span_z), rel)


def prepare(list_ref, n, first_plane, dims, rows_ref):
    depth, span_x, span_y, span_z = dims

    def attr(a):
        return list_ref[pl.ds(n * LIST + a * ROWS, ROWS), :]

    def put(slot, value):
        rows_ref[pl.ds((n * SLOTS + slot) * ROWS, ROWS), :] = value

    def along(slot, cell, weights, span):
        tile = jnp.floor(cell * (1.0 / TILE))
        low = cell - tile * float(TILE)
        for b in range(4):
            at = low + float(b)
            put(slot + b, jnp.where(at >= float(TILE), at - float(TILE), at))
            put(slot + 4 + b, weights[b])
        put(slot + 8, tile)
        put(slot + 9, jnp.where(tile >= float(span // TILE - 1), 0.0, tile + 1.0))

    along(0, attr(6), corner_weights(attr(3)), span_x)
    rounded = [w.astype(jnp.bfloat16).astype(jnp.float32) for w in corner_weights(attr(4))]
    along(10, attr(7), rounded, span_y)
    wz = corner_weights(attr(5))
    rel = from_plane(list_ref, n, first_plane, span_z)
    for z in range(depth):
        plane = jnp.zeros_like(rel)
        for a in range(4):
            plane = jnp.where(rel == float(z - a), wz[a], plane)
        put(20 + z, plane)


def build(list_ref, rows_ref, turn, dims, a_ref, b_ref):
    depth, span_x, span_y, _ = dims
    per_list = ROWS // KROWS
    n = turn // per_list
    row = (turn % per_list) * KROWS
    row_at = lax.broadcasted_iota(jnp.int32, (TILE, 128), 0).astype(jnp.float32)
    nothing = jnp.zeros((TILE, 128), jnp.bfloat16)
    for r in range(KROWS):
        lanes = pl.ds(r * 128, 128)

        def get(slot):
            return rows_ref[pl.ds((n * SLOTS + slot) * ROWS + row + r, 1), :]

        def pattern(slot):
            weights = jnp.zeros((TILE, 128), jnp.float32)
            for b in range(4):
                weights = jnp.where(row_at == get(slot + b), get(slot + 4 + b), weights)
            tiles = jnp.where(row_at >= get(slot), get(slot + 8), get(slot + 9))
            return weights, tiles.astype(jnp.bfloat16)

        wx, x_tile = pattern(0)
        forces = [list_ref[pl.ds(n * LIST + c * ROWS + row + r, 1), :] for c in range(3)]
        a_rows = [(wx * f).astype(jnp.bfloat16) for f in forces]
        for t in range(span_x // TILE):
            here = x_tile == jnp.bfloat16(t)
            for c in range(3):
                a_ref[pl.ds(c * span_x + t * TILE, TILE), lanes] = jnp.where(here, a_rows[c], nothing)
        wy, y_tile = pattern(10)
        b_rows = [(wy * get(20 + z)).astype(jnp.bfloat16) for z in range(depth)]
        for t in range(span_y // TILE):
            here = y_tile == jnp.bfloat16(t)
            for z in range(depth):
                b_ref[pl.ds(z * span_y + t * TILE, TILE), lanes] = jnp.where(here, b_rows[z], nothing)


def spread_lists(list_ref, lists, first_plane, acc_ref, dims, rows_ref):
    depth, span_x, span_y, _ = dims
    a = pltpu.VMEM((3 * span_x, KROWS * 128), jnp.bfloat16)
    b = pltpu.VMEM((depth * span_y, KROWS * 128), jnp.bfloat16)

    def run(a0, b0, a1, b1):
        spread_turns(list_ref, lists, first_plane, acc_ref, dims, rows_ref, ((a0, b0), (a1, b1)))

    touch = jnp.zeros((ROWS, 128), jnp.float32)
    for n in range(lists):
        rel = from_plane(list_ref, n, first_plane, dims[3])
        touch = jnp.where(jnp.logical_and(rel > -4.0, rel < float(depth)), 1.0, touch)

    @pl.when(jnp.max(touch) > 0.0)
    def _():
        pl.run_scoped(run, a, b, a, b)


def spread_turns(list_ref, lists, first_plane, acc_ref, dims, rows_ref, bufs):
    depth, span_x, span_y, _ = dims
    turns = lists * (ROWS // KROWS)
    for n in range(lists):
        prepare(list_ref, n, first_plane, dims, rows_ref)

    def fill(turn, which):
        build(list_ref, rows_ref, turn, dims, *bufs[which])

    def add(which):
        a_ref, b_ref = bufs[which]
        out = lax.dot_general(
            a_ref[...], b_ref[...], (((1,), (1,)), ((), ())), preferred_element_type=jnp.float32
        )
        for z in range(depth):
            acc_ref[z] += out[:, z * span_y : (z + 1) * span_y]

    fill(0, 0)

    def some_turns(i, carry):
        for u in range(UNROLL):
            fill(jnp.minimum(UNROLL * i + u + 1, turns - 1), (u + 1) % 2)
            add(u % 2)
        return carry

    lax.fori_loop(0, turns // UNROLL, some_turns, 0)


def scratch(lists):
    return [pltpu.VMEM((lists * SLOTS * ROWS, 128), jnp.float32)]


def cost(lists, dims):
    depth, span_x, span_y, _ = dims
    return pl.CostEstimate(
        flops=lists * ROWS * 128 * 3 * span_x * depth * span_y * 2,
        bytes_accessed=2000000,
        transcendentals=0,
    )


def own_plane(depth):
    return (lax.axis_index("gz") * depth).astype(jnp.float32)


def spread(markers, lists, acc, dims):
    depth, span_x, span_y, _ = dims

    def kernel(*refs):
        if acc is None:
            list_ref, out_ref, rows_ref = refs
            out_ref[...] = jnp.zeros_like(out_ref)
        else:
            list_ref, _, out_ref, rows_ref = refs
        spread_lists(list_ref, lists, own_plane(depth), out_ref, dims, rows_ref)

    operands = (in_vmem(markers),)
    if acc is not None:
        operands += (in_vmem(acc),)
    return pl.pallas_call(
        kernel,
        out_shape=pltpu.VMEM((depth, 3 * span_x, span_y), jnp.float32),
        in_specs=[vmem()] * len(operands),
        out_specs=vmem(),
        input_output_aliases={} if acc is None else {1: 0},
        scratch_shapes=scratch(lists),
        cost_estimate=cost(lists, dims),
        compiler_params=pltpu.CompilerParams(vmem_limit_bytes=KERNEL_VMEM),
        name="spread",
    )(*operands)


def spread_last(markers, lists, acc, planes, planes_at, dims):
    depth, span_x, span_y, _ = dims
    half = span_x // 2
    rows = depth * 3 * half

    def kernel(list_ref, in_ref, planes_ref, keep_ref, give_ref, acc_ref, rows_ref):
        acc_ref[...] = in_ref[...]
        give_ref[pl.ds(rows, 3 * half), :] = planes_ref[pl.ds(planes_at + 3 * half, 3 * half), :]
        spread_lists(list_ref, lists, own_plane(depth), acc_ref, dims, rows_ref)
        col = lax.axis_index("col")
        mine = pl.multiple_of(col * half, half)
        other = pl.multiple_of((1 - col) * half, half)
        for z in range(depth):
            for c in range(3):
                at = pl.ds((z * 3 + c) * half, half)
                keep_ref[at, :] = acc_ref[z, pl.ds(c * span_x + mine, half), :]
                give_ref[at, :] = acc_ref[z, pl.ds(c * span_x + other, half), :]

    return pl.pallas_call(
        kernel,
        out_shape=(
            pltpu.VMEM((rows, span_y), jnp.float32),
            pltpu.VMEM((rows + 3 * half, span_y), jnp.float32),
        ),
        in_specs=[vmem(), vmem(), vmem()],
        out_specs=(vmem(), vmem()),
        scratch_shapes=[pltpu.VMEM((depth, 3 * span_x, span_y), jnp.float32)] + scratch(lists),
        cost_estimate=cost(lists, dims),
        compiler_params=pltpu.CompilerParams(vmem_limit_bytes=KERNEL_VMEM),
        name="spread_last",
    )(in_vmem(markers), in_vmem(acc), in_vmem(planes))


def viscous_part(velocity, both):
    depth, _, half, span_y = velocity.shape
    low_at = LIST + 3 * half

    def kernel(v_ref, both_ref, base_ref):
        col = lax.axis_index("col")
        row_at = lax.broadcasted_iota(jnp.int32, (half, span_y), 0)
        for z in range(depth):
            for c in range(3):
                v = v_ref[z, c]
                x_low = both_ref[1 - col, pl.ds(low_at + z * 3 + c, 1), :]
                x_high = both_ref[1 - col, pl.ds(low_at + 3 * depth + z * 3 + c, 1), :]
                near = jnp.where(row_at == 0, x_high, pltpu.roll(v, 1, 0))
                near = near + jnp.where(row_at == half - 1, x_low, pltpu.roll(v, half - 1, 0))
                near = near + pltpu.roll(v, 1, 1) + pltpu.roll(v, span_y - 1, 1)
                if z > 0:
                    near = near + v_ref[z - 1, c]
                if z < depth - 1:
                    near = near + v_ref[z + 1, c]
                base_ref[z, c] = v + viscous * (near - 6.0 * v)

    return pl.pallas_call(
        kernel,
        out_shape=pltpu.VMEM(velocity.shape, jnp.float32),
        in_specs=[vmem(), vmem()],
        out_specs=vmem(),
        cost_estimate=pl.CostEstimate(flops=4000000, bytes_accessed=2000000, transcendentals=0),
        compiler_params=pltpu.CompilerParams(vmem_limit_bytes=KERNEL_VMEM),
        name="viscous_part",
    )(in_vmem(velocity), in_vmem(both))


def finish(keep, given, base, planes, planes_at):
    depth, _, half, span_y = base.shape
    rows = depth * 3 * half

    def kernel(keep_ref, given_ref, base_ref, planes_ref, force_hbm, next_hbm, force_ref, next_ref, sems):
        col = lax.axis_index("col")
        mine_at = jnp.where(col == 0, 0, depth - 1)
        copies = []
        for z in range(depth):
            mine = jnp.where(mine_at == z, viscous, 0.0)
            other = jnp.where(depth - 1 - mine_at == z, viscous, 0.0)
            for c in range(3):
                here = pl.ds((z * 3 + c) * half, half)
                force = keep_ref[here, :] + given_ref[1 - col, here, :]
                force_ref[z, c] = force
                base = base_ref[z, c]
                if z == 0 or z == depth - 1:
                    base = base + mine * planes_ref[pl.ds(planes_at + c * half, half), :]
                    base = base + other * given_ref[1 - col, pl.ds(rows + c * half, half), :]
                next_ref[z, c] = base + force
            copies.append(pltpu.make_async_copy(force_ref.at[z], force_hbm.at[z], sems.at[0, z]))
            copies.append(pltpu.make_async_copy(next_ref.at[z], next_hbm.at[z], sems.at[1, z]))
            copies[-2].start()
            copies[-1].start()
        for copy in copies:
            copy.wait()

    out = jax.ShapeDtypeStruct(base.shape, jnp.float32)
    return pl.pallas_call(
        kernel,
        out_shape=(out, out),
        in_specs=[vmem()] * 4,
        out_specs=(pl.BlockSpec(memory_space=pl.ANY), pl.BlockSpec(memory_space=pl.ANY)),
        scratch_shapes=[
            pltpu.VMEM(base.shape, jnp.float32),
            pltpu.VMEM(base.shape, jnp.float32),
            pltpu.SemaphoreType.DMA((2, depth)),
        ],
        compiler_params=pltpu.CompilerParams(vmem_limit_bytes=KERNEL_VMEM),
        name="finish",
    )(in_vmem(keep), in_vmem(given), in_vmem(base), in_vmem(planes))


def pack(velocity, forces, offsets, cell_x, cell_y, cell_z, band_start):
    depth, _, half, span_y = velocity.shape
    plane_rows = 3 * half
    total = LIST + plane_rows + 6 * depth

    def kernel(start_ref, v_ref, f_ref, o_ref, x_ref, y_ref, z_ref, sent_ref, plane_ref):
        for k in range(ROWS):
            for c in range(3):
                sent_ref[pl.ds(c * ROWS + k, 1), :] = f_ref[pl.ds(c, 1), pl.ds(k * 128, 128)]
                sent_ref[pl.ds((3 + c) * ROWS + k, 1), :] = o_ref[pl.ds(c, 1), pl.ds(k * 128, 128)]
        sent_ref[pl.ds(6 * ROWS, ROWS), :] = x_ref[...].astype(jnp.float32)
        sent_ref[pl.ds(7 * ROWS, ROWS), :] = y_ref[...].astype(jnp.float32)
        sent_ref[pl.ds(8 * ROWS, ROWS), :] = (z_ref[...] + start_ref[0] * depth).astype(jnp.float32)
        to_core = jnp.where(lax.axis_index("col") == 0, 0, depth - 1)
        for c in range(3):
            sent_ref[pl.ds(LIST + c * half, half), :] = v_ref[to_core, c]
            plane_ref[pl.ds(c * half, half), :] = v_ref[depth - 1 - to_core, c]
        for z in range(depth):
            for c in range(3):
                at = LIST + plane_rows + z * 3 + c
                sent_ref[pl.ds(at, 1), :] = v_ref[z, c, pl.ds(0, 1), :]
                sent_ref[pl.ds(at + 3 * depth, 1), :] = v_ref[z, c, pl.ds(half - 1, 1), :]

    return pl.pallas_call(
        kernel,
        out_shape=(
            pltpu.VMEM((total, span_y), jnp.float32),
            pltpu.VMEM((plane_rows, span_y), jnp.float32),
        ),
        in_specs=[smem()] + [vmem()] * 6,
        out_specs=(vmem(), vmem()),
        name="pack",
    )(
        band_start,
        velocity,
        forces,
        offsets,
        cell_x.reshape(ROWS, 128),
        cell_y.reshape(ROWS, 128),
        cell_z.reshape(ROWS, 128),
    )


def by_core(x, gz_count, by):
    pairs = []
    for g in range(gz_count):
        pairs.append((2 * g, 2 * ((g + by) % gz_count)))
        pairs.append((2 * g + 1, 2 * ((g - by) % gz_count) + 1))
    return lax.ppermute(x, ("gz", "col"), pairs)


def on_device(velocity, forces, offsets, cell_x, cell_y, cell_z, band_start):
    depth, _, half_x, span_y = velocity.shape
    gz_count = lax.axis_size("gz")
    col = lax.axis_index("col")
    span_x = half_x * lax.axis_size("col")
    dims = (depth, span_x, span_y, gz_count * depth)
    plane_rows = 3 * half_x
    sent, mine_out = pack(velocity, forces, offsets, cell_x, cell_y, cell_z, band_start)
    both = lax.all_gather(sent, "col", axis=0, tiled=False)
    chip = both[:, :LIST].reshape(2 * LIST, 128)
    partner = lax.dynamic_index_in_dim(both[:, LIST : LIST + plane_rows], 1 - col, 0, keepdims=False)

    second = by_core(chip, gz_count, 2)
    nearest = by_core(jnp.concatenate([chip, mine_out, partner]), gz_count, 1)
    acc = spread(sent, 1, None, dims)
    third = by_core(second, gz_count, 1)
    acc = spread(second, 2, acc, dims)
    acc = spread(nearest, 2, acc, dims)
    keep, give = spread_last(third, 2, acc, nearest, 2 * LIST, dims)
    given = lax.all_gather(give, "col", axis=0, tiled=False)
    base = viscous_part(velocity, both)
    return finish(keep, given, base, nearest, 2 * LIST)


def solution(mesh):
    in_specs = (
        P("gz", None, "col", None),
        P(None, ("gz", "col")),
        P(None, ("gz", "col")),
        P(("gz", "col")),
        P(("gz", "col")),
        P(("gz", "col")),
        P("gz"),
    )
    out_specs = (P("gz", None, "col", None), P("gz", None, "col", None))
    return jax.shard_map(
        on_device, mesh=mesh, in_specs=in_specs, out_specs=out_specs, check_vma=False
    )
```
